32 devices in a mesh: rows: 32 (over z, y, x, core).
Axes of the slice: x: 2, y: 2, z: 4, core: 2. Of those that a mesh axis runs over, the one named last changes fastest.
Arguments:
- start_panel: float32 [8, 32768], P(None, 'rows'), may hold values from -10 to 10, as said below
- diagonal_inverse: bfloat16 [32, 1024, 1024], P('rows'), may hold values from -0.6 to 12.5
- right_factor: bfloat16 [32, 1024, 1024], P('rows'), may hold values from -0.03125 to 0.03125
- left_factor: bfloat16 [32, 1024, 1024], P('rows'), may hold values from -0.03125 to 0.03125
Outputs:
- new_panels: float32 [24, 32768], P(None, 'rows')
- coefficients: float32 [3, 32, 8], replicated
- first_coefficients: float32 [3, 32, 8], replicated
The draws below stay inside these ranges and needn't reach their ends.
Inputs may be any that keep to these rules, and one draw needn't show every extreme that they name: The rows of start_panel are orthonormal under the inner product divided by 32768, up to float32 rounding.
All inputs are finite; a program needn't handle non-finite values.
Results may differ from the reference program's by a relative error of at most 0.014.
Values sent between devices are 32-bit elements; how exact they have to be, the bound alone decides.
A program may use at most 64 MiB of HBM per device.

```python
import jax
import jax.numpy as jnp
from jax import lax

BLOCK = 1024
PANEL = 8
STEPS = 3
BASIS = 32
BLOCK_ROWS = 32
UNKNOWNS = 32768
LEVELS = 5


def draw_start_panel(key, part):
    split_keys = jax.random.split(jax.random.fold_in(key, 11), 3)
    noise_rows = jnp.clip(jax.random.normal(split_keys[0], (PANEL, UNKNOWNS), jnp.float32), -6.0, 6.0)
    weights = jax.random.uniform(split_keys[1], (PANEL,), jnp.float32, -0.35, 0.35)
    common = jnp.clip(jax.random.normal(split_keys[2], (UNKNOWNS,), jnp.float32), -6.0, 6.0)
    raw = noise_rows + weights[:, None] * common[None, :]
    gram = jnp.dot(raw, raw.T, precision=lax.Precision.HIGHEST) / UNKNOWNS
    lower = jnp.linalg.cholesky(gram)
    return jax.scipy.linalg.solve_triangular(lower, raw, lower=True)


def draw_diagonal_inverse(key, part):
    split_keys = jax.random.split(jax.random.fold_in(key, 23), 2)
    spread = 0.5 * BLOCK ** (-0.5)
    position = lax.broadcasted_iota(jnp.int32, (BLOCK_ROWS, 1), 0).astype(jnp.float32) / (BLOCK_ROWS - 1)
    offdiag = spread * jnp.clip(jax.random.normal(split_keys[0], (BLOCK_ROWS, BLOCK, BLOCK), jnp.float32), -6.0, 6.0)
    diagonal = (1.0 + 2.0 * position) * jnp.exp(jax.random.uniform(split_keys[1], (BLOCK_ROWS, BLOCK), jnp.float32, -0.4, 0.4))
    identity = (lax.broadcasted_iota(jnp.int32, (BLOCK, BLOCK), 0) == lax.broadcasted_iota(jnp.int32, (BLOCK, BLOCK), 1)).astype(jnp.float32)
    return (offdiag + identity[None, :, :] * diagonal[:, :, None]).astype(jnp.bfloat16)


def block_levels(own_key, extent, pieces, smallest, top_value):
    gain = 1.0
    for dim, shards_of in pieces:
        steps = jax.random.uniform(jax.random.fold_in(jax.random.fold_in(own_key, 6), dim), (shards_of,), jnp.float32, smallest / len(pieces), top_value / len(pieces))
        gain = gain * jnp.repeat(jnp.exp(steps), extent[dim] // shards_of).reshape((-1,) + (1,) * (len(extent) - 1 - dim))
    return gain


def bell_draw(rng, extent, scale, most, shards=(), kind=jnp.bfloat16):
    drawn = scale * jax.random.normal(rng, extent, jnp.float32)
    if shards:
        drawn = drawn * block_levels(rng, extent, shards, -0.22, 0.18)
    return jnp.clip(drawn, -most, most).astype(kind)


def setup_inputs(seed: int = 0) -> dict:
    keys = jax.random.split(jax.random.key(seed), 5)
    start_panel = draw_start_panel(jax.random.fold_in(keys[4], 71), 0)
    diagonal_inverse = draw_diagonal_inverse(jax.random.fold_in(keys[4], 71), 0)
    right_factor = bell_draw(keys[2], (BLOCK_ROWS, BLOCK, BLOCK), (32 * BLOCK) ** -0.5, 0.03125, ((0, 32),))
    left_factor = bell_draw(keys[3], (BLOCK_ROWS, BLOCK, BLOCK), (32 * BLOCK) ** -0.5, 0.03125, ((0, 32),))
    return dict(start_panel=start_panel, diagonal_inverse=diagonal_inverse, right_factor=right_factor, left_factor=left_factor)


epsilon = 1e-06

def apply_rows(matrices, vectors):

    def single(couple):
        matrix, vector = couple
        return jnp.dot(vector.astype(jnp.float32), matrix.astype(jnp.float32), preferred_element_type=jnp.float32)
    return lax.map(single, (matrices, vectors))

def cyclic_solve(current, diagonal_inverse, right_factor, left_factor):
    updated = current.reshape(PANEL, BLOCK_ROWS, BLOCK).transpose(1, 0, 2)
    for height in range(LEVELS):
        distance = 2 ** height
        lowered = updated.astype(jnp.bfloat16)
        upward = apply_rows(right_factor, lowered)
        downward = apply_rows(left_factor, lowered)
        padding = jnp.zeros((distance, PANEL, BLOCK), jnp.float32)
        from_below = jnp.concatenate([padding, upward[:BLOCK_ROWS - distance]], 0)
        from_above = jnp.concatenate([downward[distance:], padding], 0)
        updated = updated - from_below - from_above
    solved = apply_rows(diagonal_inverse, updated.astype(jnp.bfloat16))
    return solved.transpose(1, 0, 2).reshape(PANEL, UNKNOWNS)

def product(left, right):
    return jnp.dot(left, right, precision=lax.Precision.HIGHEST)

def reference(start_panel, diagonal_inverse, right_factor, left_factor):
    krylov_basis = start_panel
    current = start_panel
    produced = []
    coefficients = []
    firsts = []
    for iteration in range(STEPS):
        images = cyclic_solve(current, diagonal_inverse, right_factor, left_factor)
        height = krylov_basis.shape[0]
        coef_first = product(krylov_basis, images.T) / UNKNOWNS
        projected = images - product(coef_first.T, krylov_basis)
        coef_second = product(krylov_basis, projected.T) / UNKNOWNS
        remainder = projected - product(coef_second.T, krylov_basis)
        gram_new = product(remainder, remainder.T) / UNKNOWNS + epsilon * jnp.eye(PANEL, dtype=jnp.float32)
        lower_factor = jnp.linalg.cholesky(gram_new)
        fresh = jax.scipy.linalg.solve_triangular(lower_factor, remainder, lower=True)
        column_block = jnp.zeros((BASIS, PANEL), jnp.float32)
        column_block = column_block.at[:height].set(coef_first + coef_second)
        column_block = column_block.at[height:height + PANEL].set(lower_factor.T)
        first_block = jnp.zeros((BASIS, PANEL), jnp.float32).at[:height].set(coef_first)
        produced.append(fresh)
        coefficients.append(column_block)
        firsts.append(first_block)
        krylov_basis = jnp.concatenate([krylov_basis, fresh], 0)
        current = fresh
    return (jnp.concatenate(produced, 0), jnp.stack(coefficients), jnp.stack(firsts))
```

```python
import functools

import jax
import jax.numpy as jnp
from jax import lax
from jax.experimental import pallas as pl
from jax.experimental.pallas import tpu as pltpu
from jax.sharding import PartitionSpec as P

STEPS = 3
BASIS = 32
LANES = 128
AXIS = "rows"
MESH = pl.DeviceIdType.MESH

epsilon = 1e-06


def radixes_of(count):
    sizes = []
    while count > 1:
        size = 8 if count >= 8 else count
        sizes.append(size)
        count //= size
    return sizes


def product(left, right):
    return jnp.dot(left, right, precision=lax.Precision.HIGHEST, preferred_element_type=jnp.float32)


def inner_rows(left, right):
    return lax.dot_general(
        left,
        right,
        (((1,), (1,)), ((), ())),
        precision=lax.Precision.HIGHEST,
        preferred_element_type=jnp.float32,
    )


def kernel(
    n,
    start_ref,
    diagonal_hbm,
    right_hbm,
    left_hbm,
    panels_ref,
    coef_ref,
    first_ref,
    right_w,
    left_w,
    diagonal_w,
    vectors,
    gram,
    outgoing,
    incoming,
    tiles,
    load_sem,
    send_sem,
    recv_sem,
    tile_send,
    tile_recv,
):
    me = lax.axis_index(AXIS)
    width, block = start_ref.shape
    depth = vectors.shape[0]
    unknowns = block * n
    levels = n.bit_length() - 1
    groups = []
    stride, offset = 1, 0
    for size in radixes_of(n):
        groups.append((size, stride, offset))
        stride, offset = stride * size, offset + size

    loads = [
        pltpu.make_async_copy(source.at[0], target, load_sem.at[i])
        for i, (source, target) in enumerate(
            ((right_hbm, right_w), (left_hbm, left_w), (diagonal_hbm, diagonal_w))
        )
    ]
    for load in loads:
        load.start()

    barrier = pltpu.get_barrier_semaphore()
    expected = 0
    for level in range(levels):
        distance = 2**level
        for target, present in (
            (me + distance, me + distance < n),
            (me - distance, me >= distance),
        ):
            @pl.when(present)
            def _():
                pl.semaphore_signal(barrier, inc=1, device_id=(target,), device_id_type=MESH)

            expected = expected + present.astype(jnp.int32)
    for size, stride, _ in groups:
        digit = (me // stride) % size
        for k in range(1, size):
            partner = me + ((digit + k) % size - digit) * stride
            pl.semaphore_signal(barrier, inc=1, device_id=(partner,), device_id_type=MESH)
        expected = expected + (size - 1)

    vectors[...] = jnp.zeros_like(vectors)
    vectors[pl.ds(width, width), :] = start_ref[...]
    gram[...] = jnp.zeros_like(gram)

    row = lax.broadcasted_iota(jnp.int32, (depth, depth), 0)
    col = lax.broadcasted_iota(jnp.int32, (depth, depth), 1)
    eye = (row == col).astype(jnp.float32)
    below = col < (row // width) * width
    basis_lane = lax.broadcasted_iota(jnp.int32, (width, depth), 1) >= width
    small_row = lax.broadcasted_iota(jnp.int32, (width, width), 0)
    small_col = lax.broadcasted_iota(jnp.int32, (width, width), 1)
    small_eye = (small_row == small_col).astype(jnp.float32)
    column_row = lax.broadcasted_iota(jnp.int32, (width, 1), 0)

    def widened(value):
        return jnp.concatenate(
            [value, jnp.zeros((value.shape[0], LANES - value.shape[1]), jnp.float32)], 1
        )

    def row_copy(step, level, way):
        distance = 2**level
        return pltpu.make_async_remote_copy(
            src_ref=outgoing.at[step, level, way],
            dst_ref=incoming.at[step, level, way],
            send_sem=send_sem.at[step, level, way],
            recv_sem=recv_sem.at[step, level, way],
            device_id=(me + distance if way == 0 else me - distance,),
            device_id_type=MESH,
        )

    def sends(level, way):
        distance = 2**level
        return me + distance < n if way == 0 else me >= distance

    def receives(level, way):
        return sends(level, 1 - way)

    def tile_copies(step, kind, phase):
        size, stride, offset = groups[phase]
        digit = (me // stride) % size
        copies = []
        for k in range(1, size):
            other = (digit + k) % size
            copies.append(
                pltpu.make_async_remote_copy(
                    src_ref=tiles.at[step, kind, offset + digit],
                    dst_ref=tiles.at[step, kind, offset + digit],
                    send_sem=tile_send.at[step, kind, offset + k],
                    recv_sem=tile_recv.at[step, kind, offset + digit],
                    device_id=(me + (other - digit) * stride,),
                    device_id_type=MESH,
                )
            )
        return copies

    def tile_start(step, kind, phase, value):
        size, stride, offset = groups[phase]
        digit = (me // stride) % size
        tiles[step, kind, offset + digit] = value
        for copy in tile_copies(step, kind, phase):
            copy.start()

    def tile_finish(step, kind, phase):
        size, stride, offset = groups[phase]
        digit = (me // stride) % size
        for k in range(1, size):
            other = (digit + k) % size
            pltpu.make_async_remote_copy(
                src_ref=tiles.at[step, kind, offset + digit],
                dst_ref=tiles.at[step, kind, offset + other],
                send_sem=tile_send.at[step, kind, offset + k],
                recv_sem=tile_recv.at[step, kind, offset + other],
                device_id=(me + (other - digit) * stride,),
                device_id_type=MESH,
            ).wait_recv()
        total = tiles[step, kind, offset]
        for i in range(1, size):
            total = total + tiles[step, kind, offset + i]
        return total

    loads[0].wait()
    loads[1].wait()
    loads[2].wait()
    pl.semaphore_wait(barrier, expected)

    def arnoldi_step(step, current):
        updated = current
        pending = 0
        total = None
        for level in range(levels):
            lowered = updated.astype(jnp.bfloat16)
            for way, weights in ((0, right_w), (1, left_w)):
                outgoing[step, level, way] = jnp.dot(
                    lowered, weights[...], preferred_element_type=jnp.float32
                )

                @pl.when(sends(level, way))
                def _():
                    row_copy(step, level, way).start()

            if level == 0:
                tile_start(step, 0, 0, widened(inner_rows(current, vectors[...])))
            elif pending < len(groups):
                total = tile_finish(step, 0, pending)
                pending += 1
                if pending < len(groups):
                    tile_start(step, 0, pending, total)

            for way in range(2):
                @pl.when(receives(level, way))
                def _():
                    row_copy(step, level, way).wait_recv()

                @pl.when(jnp.logical_not(receives(level, way)))
                def _():
                    incoming[step, level, way] = jnp.zeros((width, block), jnp.float32)

            updated = updated - incoming[step, level, 0] - incoming[step, level, 1]
        while pending < len(groups):
            total = tile_finish(step, 0, pending)
            pending += 1
            if pending < len(groups):
                tile_start(step, 0, pending, total)

        images = jnp.dot(
            updated.astype(jnp.bfloat16), diagonal_w[...], preferred_element_type=jnp.float32
        )
        vectors[pl.ds(0, width), :] = images
        tile_start(step, 1, 0, widened(inner_rows(images, vectors[...])))

        cross = total[:, :depth] * (1.0 / unknowns)
        cross = jnp.where(basis_lane, cross, 0.0)
        gram[pl.ds(pl.multiple_of(width * (step + 1), width), width), :] = cross
        lower = gram[...]
        full = lower + inner_rows(eye, jnp.where(below, lower, 0.0))
        excess = full - eye
        both = eye - excess
        inside = both + product(product(excess, excess), both)

        for phase in range(len(groups)):
            reduced = tile_finish(step, 1, phase)
            if phase + 1 < len(groups):
                tile_start(step, 1, phase + 1, reduced)
        reduced = reduced[:, :depth] * (1.0 / unknowns)
        coef_first = jnp.where(basis_lane, reduced, 0.0)
        combined = product(coef_first, both)
        square = (
            reduced[:, :width]
            - inner_rows(product(coef_first, inside), coef_first)
            + epsilon * small_eye
        )
        fresh = images - product(combined, vectors[...])
        factor = jnp.zeros((width, width), jnp.float32)
        for k in range(width):
            inverse = lax.rsqrt(square[k : k + 1, k : k + 1])
            column = square[:, k : k + 1] * inverse
            factor = jnp.where((small_col == k) & (small_row >= k), column, factor)
            column = jnp.where(column_row > k, column, 0.0)
            square_row = square[k : k + 1, :] * inverse
            fresh_row = fresh[k : k + 1, :] * inverse
            square = jnp.where(column_row == k, square_row, square - column * square_row)
            fresh = jnp.where(column_row == k, fresh_row, fresh - column * fresh_row)

        panels_ref[pl.ds(pl.multiple_of(width * step, width), width), :] = fresh
        first_ref[step] = widened(coef_first)
        coef_ref[step] = widened(combined) + pltpu.roll(
            widened(factor), width * (step + 2), 1
        )

        @pl.when(step + 1 < STEPS)
        def _():
            vectors[pl.ds(pl.multiple_of(width * (step + 2), width), width), :] = fresh

        for level in range(levels):
            for way in range(2):
                @pl.when(sends(level, way))
                def _():
                    row_copy(step, level, way).wait_send()
        for kind in range(2):
            for phase in range(len(groups)):
                for copy in tile_copies(step, kind, phase):
                    copy.wait_send()
        return fresh

    lax.fori_loop(0, STEPS, arnoldi_step, start_ref[...])


def body(start_panel, diagonal_inverse, right_factor, left_factor):
    n = lax.axis_size(AXIS)
    width, block = start_panel.shape
    depth = width * (STEPS + 1)
    levels = n.bit_length() - 1
    slots = sum(radixes_of(n))
    dma = pltpu.SemaphoreType.DMA
    any_space = pl.BlockSpec(memory_space=pl.ANY)
    in_vmem = pl.BlockSpec(memory_space=pltpu.VMEM)
    panels, coefs, firsts = pl.pallas_call(
        functools.partial(kernel, n),
        out_shape=(
            jax.ShapeDtypeStruct((width * STEPS, block), jnp.float32),
            jax.ShapeDtypeStruct((STEPS, width, LANES), jnp.float32),
            jax.ShapeDtypeStruct((STEPS, width, LANES), jnp.float32),
        ),
        in_specs=[in_vmem, any_space, any_space, any_space],
        out_specs=(in_vmem, in_vmem, in_vmem),
        scratch_shapes=[
            pltpu.VMEM((block, block), jnp.bfloat16),
            pltpu.VMEM((block, block), jnp.bfloat16),
            pltpu.VMEM((block, block), jnp.bfloat16),
            pltpu.VMEM((depth, block), jnp.float32),
            pltpu.VMEM((depth, depth), jnp.float32),
            pltpu.VMEM((STEPS, levels, 2, width, block), jnp.float32),
            pltpu.VMEM((STEPS, levels, 2, width, block), jnp.float32),
            pltpu.VMEM((STEPS, 2, slots, width, LANES), jnp.float32),
            dma((3,)),
            dma((STEPS, levels, 2)),
            dma((STEPS, levels, 2)),
            dma((STEPS, 2, slots)),
            dma((STEPS, 2, slots)),
        ],
        compiler_params=pltpu.CompilerParams(collective_id=0, has_side_effects=True),
    )(start_panel, diagonal_inverse, right_factor, left_factor)
    shown = slice(width, width + BASIS)
    return (
        panels,
        jnp.transpose(coefs[:, :, shown], (0, 2, 1)),
        jnp.transpose(firsts[:, :, shown], (0, 2, 1)),
    )


def solution(mesh):
    return jax.shard_map(
        body,
        mesh=mesh,
        in_specs=(
            P(None, AXIS),
            P(AXIS, None, None),
            P(AXIS, None, None),
            P(AXIS, None, None),
        ),
        out_specs=(P(None, AXIS), P(), P()),
        check_vma=False,
    )
```

```python
import functools

import jax
import jax.numpy as jnp
from jax import lax
from jax.experimental import pallas as pl
from jax.experimental.pallas import tpu as pltpu
from jax.sharding import PartitionSpec as P

STEPS = 3
BASIS = 32
LANES = 128
AXIS = "rows"
MESH = pl.DeviceIdType.MESH

epsilon = 1e-06


def radixes_of(count):
    sizes = []
    while count > 1:
        size = 8 if count >= 8 else count
        sizes.append(size)
        count //= size
    return sizes


def product(left, right):
    return jnp.dot(left, right, precision=lax.Precision.HIGHEST, preferred_element_type=jnp.float32)


def inner_rows(left, right):
    return lax.dot_general(
        left,
        right,
        (((1,), (1,)), ((), ())),
        precision=lax.Precision.HIGHEST,
        preferred_element_type=jnp.float32,
    )


def kernel(
    n,
    start_ref,
    diagonal_hbm,
    right_hbm,
    left_hbm,
    panels_ref,
    coef_ref,
    first_ref,
    right_w,
    left_w,
    diagonal_w,
    vectors,
    gram,
    outgoing,
    incoming,
    tiles,
    load_sem,
    send_sem,
    recv_sem,
    tile_send,
    tile_recv,
):
    me = lax.axis_index(AXIS)
    width, block = start_ref.shape
    depth = vectors.shape[0]
    half = block // 2
    unknowns = block * n
    levels = n.bit_length() - 1
    groups = []
    stride, offset = 1, 0
    for size in radixes_of(n):
        groups.append((size, stride, offset))
        stride, offset = stride * size, offset + size

    loads = [
        pltpu.make_async_copy(source.at[0], target, load_sem.at[i])
        for i, (source, target) in enumerate(
            ((right_hbm, right_w), (left_hbm, left_w), (diagonal_hbm, diagonal_w))
        )
    ]
    for load in loads:
        load.start()

    barrier = pltpu.get_barrier_semaphore()
    expected = 0
    for level in range(levels):
        distance = 2**level
        for target, present in (
            (me + distance, me + distance < n),
            (me - distance, me >= distance),
        ):
            @pl.when(present)
            def _():
                pl.semaphore_signal(barrier, inc=1, device_id=(target,), device_id_type=MESH)

            expected = expected + present.astype(jnp.int32)
    for size, stride, _ in groups:
        digit = (me // stride) % size
        for k in range(1, size):
            partner = me + ((digit + k) % size - digit) * stride
            pl.semaphore_signal(barrier, inc=1, device_id=(partner,), device_id_type=MESH)
        expected = expected + (size - 1)

    vectors[...] = jnp.zeros_like(vectors)
    vectors[pl.ds(width, width), :] = start_ref[...]
    gram[...] = jnp.zeros_like(gram)

    row = lax.broadcasted_iota(jnp.int32, (depth, depth), 0)
    col = lax.broadcasted_iota(jnp.int32, (depth, depth), 1)
    eye = (row == col).astype(jnp.float32)
    below = col < (row // width) * width
    basis_lane = lax.broadcasted_iota(jnp.int32, (width, depth), 1) >= width
    small_row = lax.broadcasted_iota(jnp.int32, (width, width), 0)
    small_col = lax.broadcasted_iota(jnp.int32, (width, width), 1)
    small_eye = (small_row == small_col).astype(jnp.float32)
    tile_row = lax.broadcasted_iota(jnp.int32, (width, LANES), 0)
    tile_col = lax.broadcasted_iota(jnp.int32, (width, LANES), 1)

    def widened(value):
        return jnp.concatenate(
            [value, jnp.zeros((value.shape[0], LANES - value.shape[1]), jnp.float32)], 1
        )

    def row_copy(step, level, way, part):
        distance = 2**level
        return pltpu.make_async_remote_copy(
            src_ref=outgoing.at[step, level, way, part],
            dst_ref=incoming.at[step, level, way, part],
            send_sem=send_sem.at[step, level, way, part],
            recv_sem=recv_sem.at[step, level, way, part],
            device_id=(me + distance if way == 0 else me - distance,),
            device_id_type=MESH,
        )

    def sends(level, way):
        distance = 2**level
        return me + distance < n if way == 0 else me >= distance

    def receives(level, way):
        return sends(level, 1 - way)

    def tile_copies(step, kind, phase):
        size, stride, offset = groups[phase]
        digit = (me // stride) % size
        copies = []
        for k in range(1, size):
            other = (digit + k) % size
            copies.append(
                pltpu.make_async_remote_copy(
                    src_ref=tiles.at[step, kind, offset + digit],
                    dst_ref=tiles.at[step, kind, offset + digit],
                    send_sem=tile_send.at[step, kind, offset + k],
                    recv_sem=tile_recv.at[step, kind, offset + digit],
                    device_id=(me + (other - digit) * stride,),
                    device_id_type=MESH,
                )
            )
        return copies

    def tile_start(step, kind, phase, value):
        size, stride, offset = groups[phase]
        digit = (me // stride) % size
        tiles[step, kind, offset + digit] = value
        for copy in tile_copies(step, kind, phase):
            copy.start()

    def tile_finish(step, kind, phase):
        size, stride, offset = groups[phase]
        digit = (me // stride) % size
        for k in range(1, size):
            other = (digit + k) % size
            pltpu.make_async_remote_copy(
                src_ref=tiles.at[step, kind, offset + digit],
                dst_ref=tiles.at[step, kind, offset + other],
                send_sem=tile_send.at[step, kind, offset + k],
                recv_sem=tile_recv.at[step, kind, offset + other],
                device_id=(me + (other - digit) * stride,),
                device_id_type=MESH,
            ).wait_recv()
        total = tiles[step, kind, offset]
        for i in range(1, size):
            total = total + tiles[step, kind, offset + i]
        return total

    def received(step, level, way, part):
        @pl.when(receives(level, way))
        def _():
            row_copy(step, level, way, part).wait_recv()

        @pl.when(jnp.logical_not(receives(level, way)))
        def _():
            incoming[step, level, way, part] = jnp.zeros((width, half), jnp.float32)

    def columns(part):
        return slice(part * half, (part + 1) * half)

    def partial(lowered, weights, depth_part, part):
        return jnp.dot(
            lowered,
            weights[columns(depth_part), columns(part)],
            preferred_element_type=jnp.float32,
        )

    loads[0].wait()
    loads[1].wait()
    pl.semaphore_wait(barrier, expected)

    def arnoldi_step(step, current):
        updated = [current[:, columns(part)] for part in range(2)]
        pending = 0
        total = None

        def lowered_part(level, part):
            if level > 0:
                for way in range(2):
                    received(step, level - 1, way, part)
                updated[part] = (
                    updated[part]
                    - incoming[step, level - 1, 0, part]
                    - incoming[step, level - 1, 1, part]
                )
            return updated[part].astype(jnp.bfloat16)

        for level in range(levels):
            lowered = lowered_part(level, 0)
            sums = [
                [partial(lowered, weights, 0, part) for weights in (right_w, left_w)]
                for part in range(2)
            ]
            lowered = lowered_part(level, 1)
            for part in range(2):
                for way, weights in ((0, right_w), (1, left_w)):
                    outgoing[step, level, way, part] = sums[part][way] + partial(
                        lowered, weights, 1, part
                    )
                for way in range(2):
                    @pl.when(sends(level, way))
                    def _():
                        row_copy(step, level, way, part).start()

            if level == 0:
                tile_start(step, 0, 0, widened(inner_rows(current, vectors[...])))
            elif level % 2 == 0 and pending < len(groups):
                total = tile_finish(step, 0, pending)
                pending += 1
                if pending < len(groups):
                    tile_start(step, 0, pending, total)
        while pending < len(groups):
            total = tile_finish(step, 0, pending)
            pending += 1
            if pending < len(groups):
                tile_start(step, 0, pending, total)

        @pl.when(step == 0)
        def _():
            loads[2].wait()

        lowered = lowered_part(levels, 0)
        sums = [partial(lowered, diagonal_w, 0, part) for part in range(2)]
        lowered = lowered_part(levels, 1)
        images = jnp.concatenate(
            [sums[part] + partial(lowered, diagonal_w, 1, part) for part in range(2)], 1
        )
        vectors[pl.ds(0, width), :] = images
        tile_start(step, 1, 0, widened(inner_rows(images, vectors[...])))

        cross = total[:, :depth] * (1.0 / unknowns)
        cross = jnp.where(basis_lane, cross, 0.0)
        gram[pl.ds(pl.multiple_of(width * (step + 1), width), width), :] = cross
        lower = gram[...]
        full = lower + inner_rows(eye, jnp.where(below, lower, 0.0))
        excess = full - eye
        both = eye - excess
        inside = both + product(product(excess, excess), both)

        for phase in range(len(groups)):
            reduced = tile_finish(step, 1, phase)
            if phase + 1 < len(groups):
                tile_start(step, 1, phase + 1, reduced)
        reduced = reduced[:, :depth] * (1.0 / unknowns)
        coef_first = jnp.where(basis_lane, reduced, 0.0)
        combined = product(coef_first, both)
        square = (
            reduced[:, :width]
            - inner_rows(product(coef_first, inside), coef_first)
            + epsilon * small_eye
        )
        fresh = images - product(combined, vectors[...])
        sides = [jnp.broadcast_to(square[:, k : k + 1], (width, LANES)) for k in range(width)]
        pieces = [fresh[:, at : at + LANES] for at in range(0, block, LANES)]
        factor = jnp.zeros((width, LANES), jnp.float32)
        scale = jnp.zeros((width, LANES), jnp.float32)
        for k in range(width):
            root = lax.rsqrt(jnp.broadcast_to(sides[k][k : k + 1, :], (width, LANES)))
            column = sides[k] * root
            factor = jnp.where((tile_col == k) & (tile_row >= k), column, factor)
            scale = jnp.where(tile_row == k, root, scale)
            ratio = jnp.where(tile_row > k, column * root, 0.0)
            for j in range(k + 1, width):
                sides[j] = sides[j] - ratio * sides[j][k : k + 1, :]
            pieces = [piece - ratio * piece[k : k + 1, :] for piece in pieces]
        fresh = jnp.concatenate([piece * scale for piece in pieces], 1)

        panels_ref[pl.ds(pl.multiple_of(width * step, width), width), :] = fresh
        first_ref[step] = widened(coef_first)
        coef_ref[step] = widened(combined) + pltpu.roll(
            factor, width * (step + 2), 1
        )

        @pl.when(step + 1 < STEPS)
        def _():
            vectors[pl.ds(pl.multiple_of(width * (step + 2), width), width), :] = fresh

        for level in range(levels):
            for way in range(2):
                @pl.when(sends(level, way))
                def _():
                    for part in range(2):
                        row_copy(step, level, way, part).wait_send()
        for kind in range(2):
            for phase in range(len(groups)):
                for copy in tile_copies(step, kind, phase):
                    copy.wait_send()
        return fresh

    lax.fori_loop(0, STEPS, arnoldi_step, start_ref[...])


def body(start_panel, diagonal_inverse, right_factor, left_factor):
    n = lax.axis_size(AXIS)
    width, block = start_panel.shape
    depth = width * (STEPS + 1)
    levels = n.bit_length() - 1
    slots = sum(radixes_of(n))
    dma = pltpu.SemaphoreType.DMA
    any_space = pl.BlockSpec(memory_space=pl.ANY)
    in_vmem = pl.BlockSpec(memory_space=pltpu.VMEM)
    panels, coefs, firsts = pl.pallas_call(
        functools.partial(kernel, n),
        out_shape=(
            jax.ShapeDtypeStruct((width * STEPS, block), jnp.float32),
            jax.ShapeDtypeStruct((STEPS, width, LANES), jnp.float32),
            jax.ShapeDtypeStruct((STEPS, width, LANES), jnp.float32),
        ),
        in_specs=[in_vmem, any_space, any_space, any_space],
        out_specs=(in_vmem, in_vmem, in_vmem),
        scratch_shapes=[
            pltpu.VMEM((block, block), jnp.bfloat16),
            pltpu.VMEM((block, block), jnp.bfloat16),
            pltpu.VMEM((block, block), jnp.bfloat16),
            pltpu.VMEM((depth, block), jnp.float32),
            pltpu.VMEM((depth, depth), jnp.float32),
            pltpu.VMEM((STEPS, levels, 2, 2, width, block // 2), jnp.float32),
            pltpu.VMEM((STEPS, levels, 2, 2, width, block // 2), jnp.float32),
            pltpu.VMEM((STEPS, 2, slots, width, LANES), jnp.float32),
            dma((3,)),
            dma((STEPS, levels, 2, 2)),
            dma((STEPS, levels, 2, 2)),
            dma((STEPS, 2, slots)),
            dma((STEPS, 2, slots)),
        ],
        compiler_params=pltpu.CompilerParams(collective_id=0, has_side_effects=True),
    )(start_panel, diagonal_inverse, right_factor, left_factor)
    shown = slice(width, width + BASIS)
    return (
        panels,
        jnp.transpose(coefs[:, :, shown], (0, 2, 1)),
        jnp.transpose(firsts[:, :, shown], (0, 2, 1)),
    )


def solution(mesh):
    return jax.shard_map(
        body,
        mesh=mesh,
        in_specs=(
            P(None, AXIS),
            P(AXIS, None, None),
            P(AXIS, None, None),
            P(AXIS, None, None),
        ),
        out_specs=(P(None, AXIS), P(), P()),
        check_vma=False,
    )
```

```python
import functools

import jax
import jax.numpy as jnp
from jax import lax
from jax.experimental import pallas as pl
from jax.experimental.pallas import tpu as pltpu
from jax.sharding import PartitionSpec as P

STEPS = 3
BASIS = 32
LANES = 128
GROUPS = (8, 32)
AXIS = "rows"
MESH = pl.DeviceIdType.MESH

epsilon = 1e-06


def radixes_of(count, most):
    sizes = []
    while count > 1:
        size = min(count, most)
        sizes.append(size)
        count //= size
    return sizes


def product(left, right):
    return jnp.dot(left, right, precision=lax.Precision.HIGHEST, preferred_element_type=jnp.float32)


def inner_rows(left, right):
    return lax.dot_general(
        left,
        right,
        (((1,), (1,)), ((), ())),
        precision=lax.Precision.HIGHEST,
        preferred_element_type=jnp.float32,
    )


def kernel(
    n,
    start_ref,
    diagonal_hbm,
    right_hbm,
    left_hbm,
    panels_ref,
    coef_ref,
    first_ref,
    right_w,
    left_w,
    diagonal_w,
    vectors,
    gram,
    outgoing,
    incoming,
    tiles,
    load_sem,
    send_sem,
    recv_sem,
    tile_send,
    tile_recv,
):
    me = lax.axis_index(AXIS)
    width, block = start_ref.shape
    depth = vectors.shape[0]
    half = block // 2
    unknowns = block * n
    levels = n.bit_length() - 1
    plans = []
    for most in GROUPS:
        plan, stride, offset = [], 1, 0
        for size in radixes_of(n, most):
            plan.append((size, stride, offset))
            stride, offset = stride * size, offset + size
        plans.append(plan)
    groups = plans[0]

    loads = [
        pltpu.make_async_copy(source.at[0], target, load_sem.at[i])
        for i, (source, target) in enumerate(
            ((right_hbm, right_w), (left_hbm, left_w), (diagonal_hbm, diagonal_w))
        )
    ]
    for load in loads:
        load.start()

    barrier = pltpu.get_barrier_semaphore()
    expected = 0
    for level in range(levels):
        distance = 2**level
        for target, present in (
            (me + distance, me + distance < n),
            (me - distance, me >= distance),
        ):
            @pl.when(present)
            def _():
                pl.semaphore_signal(barrier, inc=1, device_id=(target,), device_id_type=MESH)

            expected = expected + present.astype(jnp.int32)
    for size, stride, _ in plans[0] + plans[1]:
        digit = (me // stride) % size
        for k in range(1, size):
            partner = me + ((digit + k) % size - digit) * stride
            pl.semaphore_signal(barrier, inc=1, device_id=(partner,), device_id_type=MESH)
        expected = expected + (size - 1)

    vectors[...] = jnp.zeros_like(vectors)
    vectors[pl.ds(width, width), :] = start_ref[...]
    gram[...] = jnp.zeros_like(gram)

    row = lax.broadcasted_iota(jnp.int32, (depth, depth), 0)
    col = lax.broadcasted_iota(jnp.int32, (depth, depth), 1)
    eye = (row == col).astype(jnp.float32)
    below = col < (row // width) * width
    basis_lane = lax.broadcasted_iota(jnp.int32, (width, depth), 1) >= width
    small_row = lax.broadcasted_iota(jnp.int32, (width, width), 0)
    small_col = lax.broadcasted_iota(jnp.int32, (width, width), 1)
    small_eye = (small_row == small_col).astype(jnp.float32)
    tile_row = lax.broadcasted_iota(jnp.int32, (width, LANES), 0)
    tile_col = lax.broadcasted_iota(jnp.int32, (width, LANES), 1)

    def widened(value):
        return jnp.concatenate(
            [value, jnp.zeros((value.shape[0], LANES - value.shape[1]), jnp.float32)], 1
        )

    def row_copy(step, level, way, part):
        distance = 2**level
        return pltpu.make_async_remote_copy(
            src_ref=outgoing.at[step, level, way, part],
            dst_ref=incoming.at[step, level, way, part],
            send_sem=send_sem.at[step, level, way, part],
            recv_sem=recv_sem.at[step, level, way, part],
            device_id=(me + distance if way == 0 else me - distance,),
            device_id_type=MESH,
        )

    def sends(level, way):
        distance = 2**level
        return me + distance < n if way == 0 else me >= distance

    def receives(level, way):
        return sends(level, 1 - way)

    def tile_copies(step, kind, phase):
        size, stride, offset = plans[kind][phase]
        digit = (me // stride) % size
        copies = []
        for k in range(1, size):
            other = (digit + k) % size
            copies.append(
                pltpu.make_async_remote_copy(
                    src_ref=tiles.at[step, kind, offset + digit],
                    dst_ref=tiles.at[step, kind, offset + digit],
                    send_sem=tile_send.at[step, kind, offset + k],
                    recv_sem=tile_recv.at[step, kind, offset + digit],
                    device_id=(me + (other - digit) * stride,),
                    device_id_type=MESH,
                )
            )
        return copies

    def tile_start(step, kind, phase, value):
        size, stride, offset = plans[kind][phase]
        digit = (me // stride) % size
        tiles[step, kind, offset + digit] = value
        for copy in tile_copies(step, kind, phase):
            copy.start()

    def tile_finish(step, kind, phase):
        size, stride, offset = plans[kind][phase]
        digit = (me // stride) % size
        for k in range(1, size):
            other = (digit + k) % size
            pltpu.make_async_remote_copy(
                src_ref=tiles.at[step, kind, offset + digit],
                dst_ref=tiles.at[step, kind, offset + other],
                send_sem=tile_send.at[step, kind, offset + k],
                recv_sem=tile_recv.at[step, kind, offset + other],
                device_id=(me + (other - digit) * stride,),
                device_id_type=MESH,
            ).wait_recv()
        total = tiles[step, kind, offset]
        for i in range(1, size):
            total = total + tiles[step, kind, offset + i]
        return total

    def received(step, level, way, part):
        @pl.when(receives(level, way))
        def _():
            row_copy(step, level, way, part).wait_recv()

        @pl.when(jnp.logical_not(receives(level, way)))
        def _():
            incoming[step, level, way, part] = jnp.zeros((width, half), jnp.float32)

    def columns(part):
        return slice(part * half, (part + 1) * half)

    def partial(lowered, weights, depth_part, part):
        return jnp.dot(
            lowered,
            weights[columns(depth_part), columns(part)],
            preferred_element_type=jnp.float32,
        )

    loads[0].wait()
    loads[1].wait()
    pl.semaphore_wait(barrier, expected)

    def arnoldi_step(step, current):
        updated = [current[:, columns(part)] for part in range(2)]
        pending = 0
        total = None

        def lowered_part(level, part):
            if level > 0:
                for way in range(2):
                    received(step, level - 1, way, part)
                updated[part] = (
                    updated[part]
                    - incoming[step, level - 1, 0, part]
                    - incoming[step, level - 1, 1, part]
                )
            return updated[part].astype(jnp.bfloat16)

        for level in range(levels):
            lowered = lowered_part(level, 0)
            sums = [
                [partial(lowered, weights, 0, part) for weights in (right_w, left_w)]
                for part in range(2)
            ]
            lowered = lowered_part(level, 1)
            for part in range(2):
                for way, weights in ((0, right_w), (1, left_w)):
                    outgoing[step, level, way, part] = sums[part][way] + partial(
                        lowered, weights, 1, part
                    )
                for way in range(2):
                    @pl.when(sends(level, way))
                    def _():
                        row_copy(step, level, way, part).start()

            if level == 0:
                tile_start(step, 0, 0, widened(inner_rows(current, vectors[...])))
            elif level % 2 == 0 and pending < len(groups):
                total = tile_finish(step, 0, pending)
                pending += 1
                if pending < len(groups):
                    tile_start(step, 0, pending, total)
        while pending < len(groups):
            total = tile_finish(step, 0, pending)
            pending += 1
            if pending < len(groups):
                tile_start(step, 0, pending, total)

        @pl.when(step == 0)
        def _():
            loads[2].wait()

        lowered = lowered_part(levels, 0)
        sums = [partial(lowered, diagonal_w, 0, part) for part in range(2)]
        lowered = lowered_part(levels, 1)
        images = jnp.concatenate(
            [sums[part] + partial(lowered, diagonal_w, 1, part) for part in range(2)], 1
        )
        vectors[pl.ds(0, width), :] = images
        tile_start(step, 1, 0, widened(inner_rows(images, vectors[...])))

        cross = total[:, :depth] * (1.0 / unknowns)
        cross = jnp.where(basis_lane, cross, 0.0)
        gram[pl.ds(pl.multiple_of(width * (step + 1), width), width), :] = cross
        lower = gram[...]
        full = lower + inner_rows(eye, jnp.where(below, lower, 0.0))
        excess = full - eye
        both = eye - excess
        inside = both + product(product(excess, excess), both)

        for phase in range(len(plans[1])):
            reduced = tile_finish(step, 1, phase)
            if phase + 1 < len(plans[1]):
                tile_start(step, 1, phase + 1, reduced)
        reduced = reduced[:, :depth] * (1.0 / unknowns)
        coef_first = jnp.where(basis_lane, reduced, 0.0)
        combined = product(coef_first, both)
        square = (
            reduced[:, :width]
            - inner_rows(product(coef_first, inside), coef_first)
            + epsilon * small_eye
        )
        fresh = images - product(combined, vectors[...])
        sides = [jnp.broadcast_to(square[:, k : k + 1], (width, LANES)) for k in range(width)]
        pieces = [fresh[:, at : at + LANES] for at in range(0, block, LANES)]
        factor = jnp.zeros((width, LANES), jnp.float32)
        scale = jnp.zeros((width, LANES), jnp.float32)
        for k in range(width):
            root = lax.rsqrt(jnp.broadcast_to(sides[k][k : k + 1, :], (width, LANES)))
            column = sides[k] * root
            factor = jnp.where((tile_col == k) & (tile_row >= k), column, factor)
            scale = jnp.where(tile_row == k, root, scale)
            ratio = jnp.where(tile_row > k, column * root, 0.0)
            for j in range(k + 1, width):
                sides[j] = sides[j] - ratio * sides[j][k : k + 1, :]
            pieces = [piece - ratio * piece[k : k + 1, :] for piece in pieces]
        fresh = jnp.concatenate([piece * scale for piece in pieces], 1)

        panels_ref[pl.ds(pl.multiple_of(width * step, width), width), :] = fresh
        first_ref[step] = widened(coef_first)
        coef_ref[step] = widened(combined) + pltpu.roll(
            factor, width * (step + 2), 1
        )

        @pl.when(step + 1 < STEPS)
        def _():
            vectors[pl.ds(pl.multiple_of(width * (step + 2), width), width), :] = fresh

        for level in range(levels):
            for way in range(2):
                @pl.when(sends(level, way))
                def _():
                    for part in range(2):
                        row_copy(step, level, way, part).wait_send()
        for kind in range(2):
            for phase in range(len(plans[kind])):
                for copy in tile_copies(step, kind, phase):
                    copy.wait_send()
        return fresh

    lax.fori_loop(0, STEPS, arnoldi_step, start_ref[...])


def body(start_panel, diagonal_inverse, right_factor, left_factor):
    n = lax.axis_size(AXIS)
    width, block = start_panel.shape
    depth = width * (STEPS + 1)
    levels = n.bit_length() - 1
    slots = max(sum(radixes_of(n, most)) for most in GROUPS)
    dma = pltpu.SemaphoreType.DMA
    any_space = pl.BlockSpec(memory_space=pl.ANY)
    in_vmem = pl.BlockSpec(memory_space=pltpu.VMEM)
    panels, coefs, firsts = pl.pallas_call(
        functools.partial(kernel, n),
        out_shape=(
            jax.ShapeDtypeStruct((width * STEPS, block), jnp.float32),
            jax.ShapeDtypeStruct((STEPS, width, LANES), jnp.float32),
            jax.ShapeDtypeStruct((STEPS, width, LANES), jnp.float32),
        ),
        in_specs=[in_vmem, any_space, any_space, any_space],
        out_specs=(in_vmem, in_vmem, in_vmem),
        scratch_shapes=[
            pltpu.VMEM((block, block), jnp.bfloat16),
            pltpu.VMEM((block, block), jnp.bfloat16),
            pltpu.VMEM((block, block), jnp.bfloat16),
            pltpu.VMEM((depth, block), jnp.float32),
            pltpu.VMEM((depth, depth), jnp.float32),
            pltpu.VMEM((STEPS, levels, 2, 2, width, block // 2), jnp.float32),
            pltpu.VMEM((STEPS, levels, 2, 2, width, block // 2), jnp.float32),
            pltpu.VMEM((STEPS, 2, slots, width, LANES), jnp.float32),
            dma((3,)),
            dma((STEPS, levels, 2, 2)),
            dma((STEPS, levels, 2, 2)),
            dma((STEPS, 2, slots)),
            dma((STEPS, 2, slots)),
        ],
        compiler_params=pltpu.CompilerParams(collective_id=0, has_side_effects=True),
    )(start_panel, diagonal_inverse, right_factor, left_factor)
    shown = slice(width, width + BASIS)
    return (
        panels,
        jnp.transpose(coefs[:, :, shown], (0, 2, 1)),
        jnp.transpose(firsts[:, :, shown], (0, 2, 1)),
    )


def solution(mesh):
    return jax.shard_map(
        body,
        mesh=mesh,
        in_specs=(
            P(None, AXIS),
            P(AXIS, None, None),
            P(AXIS, None, None),
            P(AXIS, None, None),
        ),
        out_specs=(P(None, AXIS), P(), P()),
        check_vma=False,
    )
```
